32 devices in a mesh: dp: 16 (over z, y, x), mp: 2 (over core).
Axes of the slice: x: 2, y: 2, z: 4, core: 2. Of those that a mesh axis runs over, the one named last changes fastest.
Arguments:
- patches: bfloat16 [8192, 3200], P(('dp', 'mp')), may hold values from -120 to 120
- ln_gain: bfloat16 [3200], replicated, may hold values from 0.099609375 to 1.8984375
- ln_bias: bfloat16 [3200], replicated, may hold values from -3 to 3
- w_proj: bfloat16 [3200, 4096], P(None, 'mp'), may hold values from -0.109375 to 0.109375
- proj_bias: bfloat16 [4096], P('mp'), may hold values from -3 to 3
- rms_gain: bfloat16 [4096], replicated, may hold values from 0.099609375 to 1.8984375
- w_qkv: bfloat16 [4096, 3072], P(None, 'mp'), may hold values from -4 to 4
- image_counts: int32 [64, 8], replicated, may hold values from 1 to 16, as said below
- source_shift: int32 [32], replicated, may hold values from 0 to 15, as said below
Outputs:
- attended: bfloat16 [8192, 2048], P('dp', 'mp')
The draws below stay inside these ranges and needn't reach their ends.
Inputs may be any that keep to these rules, and one draw needn't show every extreme that they name: `image_counts`: row g holds the counts of the 8 images of tile g. In every draw all images of the tiles of some dp index hold 16 tokens. No value stands more than 2 times in source_shift, and some value stands exactly 2 times.
All inputs are finite; a program needn't handle non-finite values.
Results may differ from the reference program's by a relative error of at most 0.012.
Values may be sent and summed in bfloat16 or wider, within the bound.
A program may use at most 128 MiB of HBM per device.

```python
import math
import jax
import jax.numpy as jnp
from jax import lax

D_VIT = 3200
MODEL_WIDTH = 4096
HEAD_SIZE = 128
TILE = 128
IMG_TILE = 8
TOK_DEV = 512
QUERY_PER_KEY = 4
TILES_DEV = 4
IMG_DEV = 32
IMG_MAX = 16
TOKENS = 8192
NTILES = 64
QKV_COLS = 3072
OUT_COLS = 2048
N_DP = 16


def draw_patches(key, part):
    base_key, row_key, col_key = jax.random.split(key, 3)
    row_scale = jnp.exp(jax.random.uniform(row_key, (TOKENS, 1), jnp.float32, 0.0, math.log(10.0)))
    col_scale = jnp.exp(jax.random.uniform(col_key, (1, D_VIT), jnp.float32, math.log(0.3), math.log(3.0)))
    base_values = jax.random.normal(base_key, (TOKENS, D_VIT), jnp.float32)
    return (jnp.clip(base_values, -4.0, 4.0) * row_scale * col_scale).astype(jnp.bfloat16)


def draw_w_qkv(key, part):
    base_key = jax.random.fold_in(key, 0)
    base_values = jnp.clip(jax.random.normal(base_key, (MODEL_WIDTH, QKV_COLS), jnp.float32), -5.0, 5.0) / math.sqrt(MODEL_WIDTH)
    return jnp.clip(base_values, -4.0, 4.0).astype(jnp.bfloat16)


def draw_image_counts(key, part):
    count_key, full_key = jax.random.split(key)
    counts = jax.random.randint(count_key, (NTILES, IMG_TILE), 1, IMG_MAX + 1, dtype=jnp.int32)
    full_device = jax.random.randint(full_key, (), 0, N_DP, dtype=jnp.int32)
    owner_dev = jnp.arange(NTILES, dtype=jnp.int32) // TILES_DEV
    return jnp.where((owner_dev == full_device)[:, None], IMG_MAX, counts).astype(jnp.int32)


def draw_source_shift(key, part):
    cycle_key, order_key = jax.random.split(key)
    random_rank = jax.random.permutation(cycle_key, N_DP).astype(jnp.int32)
    values_all = jnp.arange(N_DP, dtype=jnp.int32)
    scores = jnp.where(values_all == N_DP // 2, -3, jnp.where(values_all == N_DP - 1, -2, jnp.where(values_all == 1, -1, random_rank))).astype(jnp.int32)
    cycle_order = jnp.argsort(scores, stable=True).astype(jnp.int32)
    slot_order = jax.random.permutation(order_key, IMG_DEV).astype(jnp.int32)
    return cycle_order[slot_order % N_DP].astype(jnp.int32)


def shard_levels(stream_key, shape, shards, least, top_value):
    loudness = 1.0
    for axis_at, blocks in shards:
        heights = jax.random.uniform(jax.random.fold_in(jax.random.fold_in(stream_key, 6), axis_at), (blocks,), jnp.float32, least / len(shards), top_value / len(shards))
        loudness = loudness * jnp.repeat(jnp.exp(heights), shape[axis_at] // blocks).reshape((-1,) + (1,) * (len(shape) - 1 - axis_at))
    return loudness


def scatter_about(stream_key, dims, spread, most, cuts=(), kind=jnp.bfloat16):
    drawn = spread * jax.random.normal(stream_key, dims, jnp.float32)
    if cuts:
        drawn = drawn * shard_levels(stream_key, dims, cuts, -0.22, 0.18)
    return jnp.clip(drawn, -most, most).astype(kind)


def setup_inputs(seed: int = 0) -> dict:
    key_list = jax.random.split(jax.random.key(seed), 10)
    return {
        "patches": draw_patches(jax.random.fold_in(key_list[9], 71), 0),
        "ln_gain": jnp.clip(1.0 + 0.18 * jax.random.normal(key_list[1], (D_VIT,), jnp.float32), 0.099609375, 1.8984375).astype(jnp.bfloat16),
        "ln_bias": scatter_about(key_list[2], (D_VIT,), 0.5, 3.0),
        "w_proj": scatter_about(key_list[3], (D_VIT, MODEL_WIDTH), D_VIT ** -0.5, 0.109375, ((1, 2),)),
        "proj_bias": scatter_about(key_list[4], (MODEL_WIDTH,), 0.5, 3.0, ((0, 2),)),
        "rms_gain": jnp.clip(1.0 + 0.18 * jax.random.normal(key_list[5], (MODEL_WIDTH,), jnp.float32), 0.099609375, 1.8984375).astype(jnp.bfloat16),
        "w_qkv": draw_w_qkv(jax.random.fold_in(key_list[9], 71), 0),
        "image_counts": draw_image_counts(jax.random.fold_in(key_list[9], 71), 0),
        "source_shift": draw_source_shift(jax.random.fold_in(key_list[9], 71), 0),
    }


norm_epsilon = 1e-05
rms_epsilon = 1e-05
rotary_base = 500000.0

def routing(image_counts, source_shift):
    per_dest = image_counts.reshape(N_DP, IMG_DEV)
    senders = jnp.arange(N_DP, dtype=jnp.int32)
    dest_of = jnp.mod(senders[:, None] - source_shift[None, :], N_DP).astype(jnp.int32)
    sent_counts = jnp.take_along_axis(per_dest, dest_of, axis=0).astype(jnp.int32)
    starts = (jnp.cumsum(sent_counts, axis=1) - sent_counts).astype(jnp.int32)
    slot_ends = jnp.cumsum(image_counts, axis=1).astype(jnp.int32)
    offsets = (slot_ends - image_counts).astype(jnp.int32)
    position = jnp.arange(TILE, dtype=jnp.int32)
    slot_index = lax.optimization_barrier(jnp.sum((position[None, :, None] >= slot_ends[:, None, :]).astype(jnp.int32), axis=2)).astype(jnp.int32)
    live_rows = slot_index < IMG_TILE
    clipped = jnp.minimum(slot_index, IMG_TILE - 1).astype(jnp.int32)
    inside_tile = position[None, :] - jnp.take_along_axis(offsets, clipped, axis=1)
    tile_count = jnp.arange(NTILES, dtype=jnp.int32)
    owner_dev = tile_count // TILES_DEV
    image_k = ((tile_count % TILES_DEV)[:, None] * IMG_TILE + clipped).astype(jnp.int32)
    sender = jnp.mod(owner_dev[:, None] + source_shift[image_k], N_DP).astype(jnp.int32)
    source_row = sender * TOK_DEV + starts[sender, image_k] + inside_tile
    source_row = jnp.where(live_rows, source_row, 0).astype(jnp.int32)
    return (source_row.reshape(-1), live_rows.reshape(-1), slot_index.reshape(-1))

def layer_norm(row_block, gain_vec, bias_vec):
    values = row_block.astype(jnp.float32)
    row_mean = lax.optimization_barrier(jnp.mean(values, axis=-1, keepdims=True))
    centred = values - row_mean
    row_var = lax.optimization_barrier(jnp.mean(centred * centred, axis=-1, keepdims=True))
    scaled = centred * lax.rsqrt(row_var + norm_epsilon) * gain_vec.astype(jnp.float32)
    return (scaled + bias_vec.astype(jnp.float32)).astype(jnp.bfloat16)

def rotary(values, cos_table, sine_table):
    half_width = values.shape[-1] // 2
    turned = jnp.concatenate([-values[..., half_width:], values[..., :half_width]], axis=-1)
    return values * cos_table + turned * sine_table

def attend(queries, key_rows, value_rows, segment):
    tile_count = queries.shape[0] // TILE
    groups = queries.shape[1]
    query_f = queries.reshape(tile_count, TILE, groups, QUERY_PER_KEY, HEAD_SIZE).astype(jnp.float32)
    key_f = key_rows.reshape(tile_count, TILE, groups, HEAD_SIZE).astype(jnp.float32)
    value_f = value_rows.reshape(tile_count, TILE, groups, HEAD_SIZE).astype(jnp.float32)
    scores = jnp.einsum('tqhgd,tkhd->thgqk', query_f, key_f) * HEAD_SIZE ** (-0.5)
    segments = segment.reshape(tile_count, TILE)
    position = jnp.arange(TILE, dtype=jnp.int32)
    allowed = (position[None, :, None] >= position[None, None, :]) & (segments[:, :, None] == segments[:, None, :])
    scores = jnp.where(allowed[:, None, None], scores, -1e+30)
    row_max = lax.optimization_barrier(jnp.max(scores, axis=-1, keepdims=True))
    weights = jnp.exp(scores - row_max)
    probabilities = (weights / lax.optimization_barrier(jnp.sum(weights, axis=-1, keepdims=True))).astype(jnp.bfloat16)
    attended = jnp.einsum('thgqk,tkhd->tqhgd', probabilities.astype(jnp.float32), value_f)
    return attended.reshape(tile_count * TILE, groups * QUERY_PER_KEY * HEAD_SIZE)

def finish(hidden, live_flat, segment, rms_gain, w_qkv):
    row_total = hidden.shape[0]
    widened = hidden.astype(jnp.float32)
    mean_square = lax.optimization_barrier(jnp.mean(widened * widened, axis=-1, keepdims=True))
    rms_normed = (widened * lax.rsqrt(mean_square + rms_epsilon) * rms_gain.astype(jnp.float32)).astype(jnp.bfloat16)
    projections = jnp.dot(rms_normed, w_qkv, preferred_element_type=jnp.float32)
    groups = w_qkv.shape[1] // ((QUERY_PER_KEY + 2) * HEAD_SIZE)
    projections = projections.reshape(row_total, groups, QUERY_PER_KEY + 2, HEAD_SIZE)
    position = (jnp.arange(row_total, dtype=jnp.int32) % TILE).astype(jnp.float32)
    frequency = rotary_base ** (-(jnp.arange(HEAD_SIZE // 2, dtype=jnp.float32) * (2.0 / HEAD_SIZE)))
    angles = position[:, None] * frequency[None, :]
    cos_table = jnp.concatenate([jnp.cos(angles), jnp.cos(angles)], axis=-1)[:, None, None, :]
    sine_table = jnp.concatenate([jnp.sin(angles), jnp.sin(angles)], axis=-1)[:, None, None, :]
    queries = rotary(projections[:, :, :QUERY_PER_KEY], cos_table, sine_table).astype(jnp.bfloat16)
    key_rows = rotary(projections[:, :, QUERY_PER_KEY], cos_table[:, :, 0], sine_table[:, :, 0]).astype(jnp.bfloat16)
    value_rows = projections[:, :, QUERY_PER_KEY + 1].astype(jnp.bfloat16)
    attended = attend(queries, key_rows, value_rows, segment).astype(jnp.bfloat16)
    return jnp.where(live_flat[:, None], attended, jnp.zeros_like(attended))

def reference(patches, ln_gain, ln_bias, w_proj, proj_bias, rms_gain, w_qkv, image_counts, source_shift):
    source_row, live_rows, slot_index = routing(image_counts, source_shift)

    def device_block(device):
        pick_rows = lax.dynamic_slice_in_dim(source_row, device * TOK_DEV, TOK_DEV)
        live_flat = lax.dynamic_slice_in_dim(live_rows, device * TOK_DEV, TOK_DEV)
        segment = lax.dynamic_slice_in_dim(slot_index, device * TOK_DEV, TOK_DEV)
        gathered = jnp.take(patches, pick_rows, axis=0)
        normed = layer_norm(gathered, ln_gain, ln_bias)
        pre_act = jnp.dot(normed, w_proj, preferred_element_type=jnp.float32) + proj_bias.astype(jnp.float32)
        activated = jax.nn.gelu(pre_act, approximate=False)
        hidden = jnp.where(live_flat[:, None], activated, jnp.zeros_like(activated)).astype(jnp.bfloat16)
        return finish(hidden, live_flat, segment, rms_gain, w_qkv)
    blocks = lax.map(device_block, jnp.arange(N_DP, dtype=jnp.int32))
    return blocks.reshape(TOKENS, OUT_COLS)
```

```python
import functools

import jax
import jax.numpy as jnp
import numpy as np
from jax import lax
from jax.experimental import pallas as pl
from jax.experimental.pallas import tpu as pltpu
from jax.sharding import PartitionSpec as P

HEAD_SIZE = 128
TILE = 128
QUERY_PER_KEY = 4
COL_TILE = 256
CHUNK = 256

norm_epsilon = 1e-05
rms_epsilon = 1e-05
rotary_base = 500000.0

F32 = jnp.float32
BF16 = jnp.bfloat16
MESH = pl.DeviceIdType.MESH


def shift_order(senders):
    return sorted(range(senders), key=lambda v: (abs(v - senders // 2), v))


def rotary_parts():
    frequency = np.float32(rotary_base) ** (
        -(np.arange(HEAD_SIZE // 2, dtype=np.float32) * np.float32(2.0 / HEAD_SIZE))
    )
    angles = np.arange(TILE, dtype=np.float32)[:, None] * frequency[None, :].astype(np.float32)
    cos = np.cos(angles.astype(np.float64)).astype(np.float32)
    sin = np.sin(angles.astype(np.float64)).astype(np.float32)
    parts = []
    for table in (np.concatenate([cos, cos], 1), np.concatenate([-sin, sin], 1)):
        rest = table
        for _ in range(3):
            term = rest.astype(jnp.bfloat16)
            parts.append(term)
            rest = rest - term.astype(np.float32)
    return np.concatenate(parts, axis=1)


def gelu(v):
    return 0.5 * v * (1.0 + lax.erf(v * np.float32(0.5**0.5)))


def iota(shape, axis):
    return lax.broadcasted_iota(jnp.int32, shape, axis)


def lane_sum(x):
    return jnp.sum(x, axis=1, keepdims=True)


def kernel(
    senders,
    order,
    patches,
    ln_gain,
    ln_bias,
    proj_bias,
    rms_gain,
    per_dest,
    shift_col,
    table,
    w_proj,
    w_qkv,
    out,
    w1,
    w2,
    normed,
    picked,
    hidden,
    rms_normed,
    proj,
    outbox,
    inbox,
    w1_sem,
    w2_sem,
    norm_sems,
    hid_send,
    hid_recv,
    a2a_send,
    a2a_recv,
):
    me = lax.axis_index("dp")
    core = lax.axis_index("mp")
    peer = 1 - core
    half, d_vit = patches.shape
    rows = 2 * half
    box_rows = outbox.shape[0]
    block = box_rows // senders
    images = shift_col.shape[0]
    tiles_dev = rows // TILE
    img_tile = images // tiles_dev
    img_most = TILE // img_tile
    pair_slots = block // img_most
    chunks = box_rows // CHUNK
    half_cols = w_proj.shape[1]
    qkv_cols = w_qkv.shape[1]
    groups = qkv_cols // ((QUERY_PER_KEY + 2) * HEAD_SIZE)
    tiles1 = half_cols // COL_TILE
    tiles2 = qkv_cols // COL_TILE

    barrier = pltpu.get_barrier_semaphore()
    pl.semaphore_signal(barrier, inc=1, device_id={"mp": peer}, device_id_type=MESH)
    for v in range(1, senders):
        pl.semaphore_signal(
            barrier, inc=1, device_id={"dp": lax.rem(me + v, senders)}, device_id_type=MESH
        )

    def w1_copy(j):
        cols = pl.ds(pl.multiple_of(j * COL_TILE, COL_TILE), COL_TILE)
        return pltpu.make_async_copy(w_proj.at[:, cols], w1.at[:, cols], w1_sem.at[j])

    def w2_copy(j):
        cols = pl.ds(pl.multiple_of(j * COL_TILE, COL_TILE), COL_TILE)
        return pltpu.make_async_copy(w_qkv.at[:, cols], w2.at[:, cols], w2_sem.at[j])

    for j in range(tiles1):
        w1_copy(j).start()
    for j in range(tiles2):
        w2_copy(j).start()

    gain_f = ln_gain[...].astype(F32)
    bias_f = ln_bias[...].astype(F32)
    base = pl.multiple_of(core * half, half)

    @pl.loop(0, half // 16)
    def _(r):
        at = pl.ds(pl.multiple_of(r * 16, 16), 16)
        values = patches[at, :].astype(F32)
        centred = values - jnp.mean(values, axis=-1, keepdims=True)
        variance = jnp.mean(centred * centred, axis=-1, keepdims=True)
        scaled = centred * lax.rsqrt(variance + norm_epsilon) * gain_f + bias_f
        normed[pl.ds(pl.multiple_of(base + r * 16, 16), 16), :] = scaled.astype(BF16)

    pl.semaphore_wait(barrier, senders)

    mine = normed.at[pl.ds(base, half)]
    norm_copy = pltpu.make_async_remote_copy(
        src_ref=mine,
        dst_ref=mine,
        send_sem=norm_sems.at[0],
        recv_sem=norm_sems.at[1],
        device_id={"mp": peer},
        device_id_type=MESH,
    )
    norm_copy.start()

    sq = (images, images)
    k_at, l_at = iota(sq, 0), iota(sq, 1)
    eye = k_at == l_at
    before = l_at < k_at
    same_tile = (k_at // img_tile) == (l_at // img_tile)

    def to_row(col):
        return jnp.sum(jnp.where(eye, col, 0), axis=0, keepdims=True)

    shift = shift_col[...]
    dest = me - shift
    dest = jnp.where(dest < 0, dest + senders, dest)
    counts_to = jnp.zeros(sq, jnp.int32)
    place = jnp.zeros((images, 1), jnp.int32)
    for v in range(senders):
        counts_to = jnp.where(dest == v, per_dest[v : v + 1, :], counts_to)
        place = jnp.where(shift == order[v], v, place)
    sent_row = jnp.sum(jnp.where(eye, counts_to, 0), axis=0, keepdims=True)
    starts = lane_sum(jnp.where(before, sent_row, 0))
    far_offset = lane_sum(jnp.where(before & same_tile, counts_to, 0))
    shift_row = to_row(shift)
    rank = lane_sum(jnp.where(before & (shift_row == shift), 1, 0))
    slot_row = to_row(place * pair_slots + rank)
    starts_row = to_row(starts)
    far_row = to_row(far_offset)

    dest_at = iota(per_dest.shape, 0)
    my_row = jnp.sum(jnp.where(dest_at == me, per_dest[...], 0), axis=0, keepdims=True)
    my_offset = lane_sum(jnp.where(before & same_tile, my_row, 0))
    my_off_row = to_row(my_offset)

    box_at = (CHUNK, images)

    def of_chunk(c):
        row_at = iota(box_at, 0) + c * CHUNK
        hit = slot_row == row_at // img_most
        inside = (iota((CHUNK, 1), 0) + c * CHUNK) % img_most
        src = lane_sum(jnp.where(hit, starts_row, 0)) + inside
        pos = lane_sum(jnp.where(hit, far_row, 0)) + inside
        return src, pos

    def copy_hidden(c):
        ref = hidden.at[core, pl.ds(c * CHUNK, CHUNK)]
        return pltpu.make_async_remote_copy(
            src_ref=ref,
            dst_ref=ref,
            send_sem=hid_send.at[c],
            recv_sem=hid_recv.at[c],
            device_id={"mp": peer},
            device_id_type=MESH,
        )

    def copy_block(o):
        at = pl.ds(o * block, block)
        return pltpu.make_async_remote_copy(
            src_ref=outbox.at[at],
            dst_ref=inbox.at[at],
            send_sem=a2a_send.at[o],
            recv_sem=a2a_recv.at[o],
            device_id={"dp": lax.rem(me + senders - order[o], senders)},
            device_id_type=MESH,
        )

    pick_tile = 128 * max(w for w in range(1, 9) if (d_vit // 128) % w == 0)
    chunk_rows = [of_chunk(c) for c in range(chunks)]
    norm_copy.wait_recv()

    def project(c):
        select = jnp.where(iota((CHUNK, rows), 1) == chunk_rows[c][0], 1.0, 0.0).astype(BF16)

        @pl.loop(0, d_vit // pick_tile)
        def _(j):
            cols = pl.ds(pl.multiple_of(j * pick_tile, pick_tile), pick_tile)
            picked[:, cols] = jnp.dot(
                select, normed[:, cols], preferred_element_type=F32
            ).astype(BF16)

        @pl.loop(0, tiles1)
        def _(j):
            if c == 0:
                w1_copy(j).wait()
            cols = pl.ds(pl.multiple_of(j * COL_TILE, COL_TILE), COL_TILE)
            pre = jnp.dot(picked[...], w1[:, cols], preferred_element_type=F32)
            pre = pre + proj_bias[:, cols].astype(F32)
            hidden[core, pl.ds(c * CHUNK, CHUNK), cols] = gelu(pre).astype(BF16)

        copy_hidden(c).start()

    q_at = iota((QUERY_PER_KEY * TILE, TILE), 0) % TILE
    s_at = iota((QUERY_PER_KEY * TILE, TILE), 1)
    allowed = (q_at // img_most == s_at // img_most) & (s_at <= q_at)

    def finish(c):
        copy_hidden(c).wait_recv()
        pos_hot = jnp.where(iota((CHUNK, TILE), 1) == chunk_rows[c][1], 1.0, 0.0).astype(BF16)
        terms = jnp.dot(pos_hot, table[...], preferred_element_type=F32)
        w = HEAD_SIZE
        cos = terms[:, :w] + terms[:, w : 2 * w] + terms[:, 2 * w : 3 * w]
        sin = terms[:, 3 * w : 4 * w] + terms[:, 4 * w : 5 * w] + terms[:, 5 * w :]

        @pl.loop(0, CHUNK // 16)
        def _(r):
            at = pl.ds(pl.multiple_of(c * CHUNK + r * 16, 16), 16)
            to = pl.ds(pl.multiple_of(r * 16, 16), 16)
            total = jnp.zeros((16, 1), F32)
            for h in range(2):
                x = hidden[h, at, :].astype(F32)
                total = total + jnp.sum(x * x, axis=-1, keepdims=True)
            scale = lax.rsqrt(total * (1.0 / (2 * half_cols)) + rms_epsilon)
            for h in range(2):
                x = hidden[h, at, :].astype(F32)
                g = rms_gain[:, h * half_cols : (h + 1) * half_cols].astype(F32)
                rms_normed[to, h * half_cols : (h + 1) * half_cols] = (x * scale * g).astype(BF16)

        @pl.loop(0, tiles2)
        def _(j):
            if c == 0:
                w2_copy(j).wait()
            cols = pl.ds(pl.multiple_of(j * COL_TILE, COL_TILE), COL_TILE)
            proj[:, cols] = jnp.dot(rms_normed[...], w2[:, cols], preferred_element_type=F32)

        def head(first, h, rotate):
            v = proj[first : first + TILE, h * w : (h + 1) * w]
            if rotate:
                v = v * cos[first : first + TILE] + pltpu.roll(v, w // 2, 1) * sin[first : first + TILE]
            return v.astype(BF16)

        for first in range(0, CHUNK, TILE):
            for g in range(groups):
                h0 = g * (QUERY_PER_KEY + 2)
                q = jnp.concatenate(
                    [head(first, h0 + i, True) for i in range(QUERY_PER_KEY)], axis=0
                )
                k = head(first, h0 + QUERY_PER_KEY, True)
                v = head(first, h0 + QUERY_PER_KEY + 1, False)
                scores = lax.dot_general(
                    q, k, (((1,), (1,)), ((), ())), preferred_element_type=F32
                ) * np.float32(HEAD_SIZE ** (-0.5))
                scores = jnp.where(allowed, scores, -1e30)
                weights = jnp.exp(scores - jnp.max(scores, axis=-1, keepdims=True))
                probs = (weights / jnp.sum(weights, axis=-1, keepdims=True)).astype(BF16)
                got = jnp.dot(probs, v, preferred_element_type=F32).astype(BF16)
                for i in range(QUERY_PER_KEY):
                    a = (g * QUERY_PER_KEY + i) * w
                    outbox[c * CHUNK + first : c * CHUNK + first + TILE, a : a + w] = got[
                        i * TILE : (i + 1) * TILE
                    ]
        for o in range(c * CHUNK // block, (c + 1) * CHUNK // block):
            if o < senders - 1:
                copy_block(o).start()
        if c == chunks - 1:
            inbox[box_rows - block :, :] = outbox[box_rows - block :, :]

    for c in range(chunks):
        project(c)
        if c > 0:
            finish(c - 1)
    finish(chunks - 1)

    t_at = iota((TILE, images), 0)
    image_at = iota((TILE, images), 1)
    place_of = []
    for t in range(tiles_dev):
        hit = (image_at // img_tile == t) & (t_at >= my_off_row) & (t_at < my_off_row + my_row)
        at = jnp.where(hit, slot_row * img_most + (t_at - my_off_row) + 1, 0)
        place_of.append(lane_sum(at) - 1)

    for o in range(senders - 1):
        copy_block(o).wait_recv()
    for t in range(tiles_dev):
        select = jnp.where(iota((TILE, box_rows), 1) == place_of[t], 1.0, 0.0).astype(BF16)
        out[t * TILE : (t + 1) * TILE, :] = jnp.dot(
            select, inbox[...], preferred_element_type=F32
        ).astype(BF16)

    norm_copy.wait_send()
    for c in range(chunks):
        copy_hidden(c).wait_send()
    for o in range(senders - 1):
        copy_block(o).wait_send()


def local(
    patches, ln_gain, ln_bias, w_proj, proj_bias, rms_gain, w_qkv, image_counts, source_shift
):
    senders = lax.axis_size("dp")
    order = shift_order(senders)
    half, d_vit = patches.shape
    rows = 2 * half
    half_cols = w_proj.shape[1]
    qkv_cols = w_qkv.shape[1]
    groups = qkv_cols // ((QUERY_PER_KEY + 2) * HEAD_SIZE)
    out_cols = groups * QUERY_PER_KEY * HEAD_SIZE
    images = source_shift.shape[0]
    img_most = TILE // (images // (rows // TILE))
    pair_slots = (images + senders - 1) // senders
    box_rows = senders * pair_slots * img_most
    chunks = box_rows // CHUNK
    vmem = pl.BlockSpec(memory_space=pltpu.VMEM)
    hbm = pl.BlockSpec(memory_space=pl.ANY)
    dma = pltpu.SemaphoreType.DMA
    return pl.pallas_call(
        functools.partial(kernel, senders, order),
        out_shape=jax.ShapeDtypeStruct((rows, out_cols), BF16),
        in_specs=[vmem] * 8 + [hbm] * 2,
        out_specs=vmem,
        scratch_shapes=[
            pltpu.VMEM(w_proj.shape, BF16),
            pltpu.VMEM(w_qkv.shape, BF16),
            pltpu.VMEM((rows, d_vit), BF16),
            pltpu.VMEM((CHUNK, d_vit), BF16),
            pltpu.VMEM((2, box_rows, half_cols), BF16),
            pltpu.VMEM((CHUNK, 2 * half_cols), BF16),
            pltpu.VMEM((CHUNK, qkv_cols), F32),
            pltpu.VMEM((box_rows, out_cols), BF16),
            pltpu.VMEM((box_rows, out_cols), BF16),
            dma((half_cols // COL_TILE,)),
            dma((qkv_cols // COL_TILE,)),
            dma((2,)),
            dma((chunks,)),
            dma((chunks,)),
            dma((senders,)),
            dma((senders,)),
        ],
        compiler_params=pltpu.CompilerParams(
            collective_id=0, has_side_effects=True, vmem_limit_bytes=60 * 1024 * 1024
        ),
        name="projector_attention",
    )(
        patches,
        ln_gain.reshape(1, -1),
        ln_bias.reshape(1, -1),
        proj_bias.reshape(1, -1),
        rms_gain.reshape(1, -1),
        image_counts.reshape(senders, images),
        source_shift.reshape(images, 1),
        jnp.asarray(rotary_parts()),
        w_proj,
        w_qkv,
    )


def solution(mesh):
    in_specs = (
        P(("dp", "mp"), None),
        P(),
        P(),
        P(None, "mp"),
        P("mp"),
        P(),
        P(None, "mp"),
        P(),
        P(),
    )
    out_specs = P("dp", "mp")
    return jax.shard_map(local, mesh=mesh, in_specs=in_specs, out_specs=out_specs, check_vma=False)
```

```python
import functools

import jax
import jax.numpy as jnp
import numpy as np
from jax import lax
from jax.experimental import pallas as pl
from jax.experimental.pallas import tpu as pltpu
from jax.sharding import PartitionSpec as P

HEAD_SIZE = 128
TILE = 128
QUERY_PER_KEY = 4
COL_TILE = 256
CHUNKS = (256, 256)

norm_epsilon = 1e-05
rms_epsilon = 1e-05
rotary_base = 500000.0

F32 = jnp.float32
BF16 = jnp.bfloat16
MESH = pl.DeviceIdType.MESH


def shift_order(senders):
    return sorted(range(senders), key=lambda v: (abs(v - senders // 2), v))


def rotary_parts():
    frequency = np.float32(rotary_base) ** (
        -(np.arange(HEAD_SIZE // 2, dtype=np.float32) * np.float32(2.0 / HEAD_SIZE))
    )
    angles = np.arange(TILE, dtype=np.float32)[:, None] * frequency[None, :].astype(np.float32)
    cos = np.cos(angles.astype(np.float64)).astype(np.float32)
    sin = np.sin(angles.astype(np.float64)).astype(np.float32)
    parts = []
    for table in (np.concatenate([cos, cos], 1), np.concatenate([-sin, sin], 1)):
        rest = table
        for _ in range(3):
            term = rest.astype(jnp.bfloat16)
            parts.append(term)
            rest = rest - term.astype(np.float32)
    return np.concatenate(parts, axis=1)


def chunk_list(box_rows):
    sizes = list(CHUNKS)
    while sum(sizes) < box_rows:
        sizes.append(CHUNKS[-1])
    return sizes


def gelu(v):
    return 0.5 * v * (1.0 + lax.erf(v * np.float32(0.5**0.5)))


def iota(shape, axis):
    return lax.broadcasted_iota(jnp.int32, shape, axis)


def lane_sum(x):
    return jnp.sum(x, axis=1, keepdims=True)


def kernel(
    senders,
    order,
    ln_gain,
    ln_bias,
    proj_bias,
    rms_gain,
    counts,
    source_shift,
    table,
    patches,
    w_proj,
    w_qkv,
    out,
    raw,
    w1,
    w2,
    normed,
    picked,
    hidden,
    rms_normed,
    pre,
    bias,
    proj,
    outbox,
    inbox,
    placed,
    raw_sem,
    out_sem,
    w1_sem,
    w2_sem,
    norm_send,
    norm_recv,
    hid_send,
    hid_recv,
    a2a_send,
    a2a_recv,
):
    me = lax.axis_index("dp")
    core = lax.axis_index("mp")
    peer = 1 - core
    half, d_vit = raw.shape
    rows = 2 * half
    box_rows = outbox.shape[0]
    block = box_rows // senders
    images = source_shift.shape[0]
    tiles_dev = rows // TILE
    img_tile = images // tiles_dev
    img_most = TILE // img_tile
    pair_slots = block // img_most
    sizes = chunk_list(box_rows)
    chunks = len(sizes)
    firsts = [sum(sizes[:c]) for c in range(chunks)]
    half_cols = w_proj.shape[1]
    qkv_cols = w_qkv.shape[1]
    groups = qkv_cols // ((QUERY_PER_KEY + 2) * HEAD_SIZE)
    tiles1 = half_cols // COL_TILE
    tiles2 = qkv_cols // COL_TILE

    part = half // 2

    def raw_copy(i):
        at = pl.ds(i * part, part)
        return pltpu.make_async_copy(patches.at[at], raw.at[at], raw_sem.at[i])

    for i in range(2):
        raw_copy(i).start()

    barrier = pltpu.get_barrier_semaphore()
    pl.semaphore_signal(barrier, inc=1, device_id={"mp": peer}, device_id_type=MESH)
    for v in range(1, senders):
        pl.semaphore_signal(
            barrier, inc=1, device_id={"dp": lax.rem(me + v, senders)}, device_id_type=MESH
        )

    def w1_copy(j):
        cols = pl.ds(pl.multiple_of(j * COL_TILE, COL_TILE), COL_TILE)
        return pltpu.make_async_copy(w_proj.at[:, cols], w1.at[:, cols], w1_sem.at[j])

    def w2_copy(j):
        cols = pl.ds(pl.multiple_of(j * COL_TILE, COL_TILE), COL_TILE)
        return pltpu.make_async_copy(w_qkv.at[:, cols], w2.at[:, cols], w2_sem.at[j])

    gain_f = ln_gain[...].reshape(1, -1).astype(F32)
    bias_f = ln_bias[...].reshape(1, -1).astype(F32)

    def norm_copy(i):
        mine = normed.at[pl.ds(pl.multiple_of(core * half + i * part, part), part)]
        return pltpu.make_async_remote_copy(
            src_ref=mine,
            dst_ref=mine,
            send_sem=norm_send.at[i],
            recv_sem=norm_recv.at[i],
            device_id={"mp": peer},
            device_id_type=MESH,
        )

    for i in range(2):
        raw_copy(i).wait()
        if i == 0:
            for j in range(tiles1):
                w1_copy(j).start()
            for j in range(tiles2):
                w2_copy(j).start()

        @pl.loop(0, part // 16, unroll=2)
        def _(r):
            values = raw[pl.ds(pl.multiple_of(i * part + r * 16, 16), 16), :].astype(F32)
            centred = values - jnp.mean(values, axis=-1, keepdims=True)
            variance = jnp.mean(centred * centred, axis=-1, keepdims=True)
            scaled = centred * lax.rsqrt(variance + norm_epsilon) * gain_f + bias_f
            to = pl.ds(pl.multiple_of(core * half + i * part + r * 16, 16), 16)
            normed[to, :] = scaled.astype(BF16)

        if i == 0:
            pl.semaphore_wait(barrier, senders)
        norm_copy(i).start()

    sq = (images, images)
    k_at, l_at = iota(sq, 0), iota(sq, 1)
    eye = k_at == l_at
    before = l_at < k_at
    same_tile = (k_at // img_tile) == (l_at // img_tile)

    def to_row(col):
        return jnp.sum(jnp.where(eye, col, 0), axis=0, keepdims=True)

    tiles_all = counts.shape[1]
    spread = (iota((img_tile, images), 1) % img_tile == iota((img_tile, images), 0)).astype(F32)
    wide = lax.dot_general(
        counts[...].astype(F32).astype(BF16),
        spread.astype(BF16),
        (((0,), (0,)), ((), ())),
        preferred_element_type=F32,
    )
    own_tile = iota((tiles_all, images), 1) // img_tile == iota((tiles_all, images), 0) % tiles_dev
    wide = jnp.where(own_tile, wide, 0.0).astype(BF16)
    gather = (iota((senders, tiles_all), 1) // tiles_dev == iota((senders, tiles_all), 0)).astype(F32)
    per_dest = jnp.dot(gather.astype(BF16), wide, preferred_element_type=F32).astype(jnp.int32)

    shift_row = source_shift[...].reshape(1, images)
    shift = lane_sum(jnp.where(eye, shift_row, 0))
    dest = me - shift
    dest = jnp.where(dest < 0, dest + senders, dest)
    counts_to = jnp.zeros(sq, jnp.int32)
    place = jnp.zeros((images, 1), jnp.int32)
    for v in range(senders):
        counts_to = jnp.where(dest == v, per_dest[v : v + 1, :], counts_to)
        place = jnp.where(shift == order[v], v, place)
    sent_row = jnp.sum(jnp.where(eye, counts_to, 0), axis=0, keepdims=True)
    starts = lane_sum(jnp.where(before, sent_row, 0))
    far_offset = lane_sum(jnp.where(before & same_tile, counts_to, 0))
    rank = lane_sum(jnp.where(before & (shift_row == shift), 1, 0))
    slot_row = to_row(place * pair_slots + rank)
    starts_row = to_row(starts)
    far_row = to_row(far_offset)

    dest_at = iota(per_dest.shape, 0)
    my_row = jnp.sum(jnp.where(dest_at == me, per_dest, 0), axis=0, keepdims=True)
    my_offset = lane_sum(jnp.where(before & same_tile, my_row, 0))
    my_off_row = to_row(my_offset)

    def of_chunk(c):
        row_at = iota((sizes[c], images), 0) + firsts[c]
        hit = slot_row == row_at // img_most
        inside = iota((sizes[c], 1), 0) % img_most
        src = lane_sum(jnp.where(hit, starts_row, 0)) + inside
        pos = lane_sum(jnp.where(hit, far_row, 0)) + inside
        return src, pos

    def copy_hidden(c, part):
        ref = hidden.at[
            core, pl.ds(firsts[c], sizes[c]), pl.ds(part * half_cols // 2, half_cols // 2)
        ]
        return pltpu.make_async_remote_copy(
            src_ref=ref,
            dst_ref=ref,
            send_sem=hid_send.at[2 * c + part],
            recv_sem=hid_recv.at[2 * c + part],
            device_id={"mp": peer},
            device_id_type=MESH,
        )

    def copy_block(o):
        at = pl.ds(o * block, block)
        return pltpu.make_async_remote_copy(
            src_ref=outbox.at[at],
            dst_ref=inbox.at[at],
            send_sem=a2a_send.at[o],
            recv_sem=a2a_recv.at[o],
            device_id={"dp": lax.rem(me + senders - order[o], senders)},
            device_id_type=MESH,
        )

    pick_tile = 128 * max(w for w in range(1, 9) if (d_vit // 128) % w == 0)
    chunk_rows = [of_chunk(c) for c in range(chunks)]
    for i in range(2):
        norm_copy(i).wait_recv()

    def project(c):
        size = sizes[c]
        rows_at = pl.ds(firsts[c], size)
        select = jnp.where(iota((size, rows), 1) == chunk_rows[c][0], 1.0, 0.0).astype(BF16)

        @pl.loop(0, d_vit // pick_tile)
        def _(j):
            cols = pl.ds(pl.multiple_of(j * pick_tile, pick_tile), pick_tile)
            picked[:size, cols] = jnp.dot(
                select, normed[:, cols], preferred_element_type=F32
            ).astype(BF16)

        def columns(j):
            return pl.ds(pl.multiple_of(j * COL_TILE, COL_TILE), COL_TILE)

        def multiply(j, slot):
            if c == 0:
                w1_copy(j).wait()
            pre[slot, :size] = jnp.dot(
                picked[:size], w1[:, columns(j)], preferred_element_type=F32
            )

        bias_row = proj_bias[...].reshape(1, -1)

        def activate(j, slot):
            x = pre[slot, :size] + bias[:, columns(j)]
            hidden[core, rows_at, columns(j)] = gelu(x).astype(BF16)

        if c == 0:
            bias[...] = bias_row.astype(F32)
        multiply(0, 0)
        pairs = tiles1 // 2
        for part in range(2):
            low, high = part * pairs // 2, (part + 1) * pairs // 2 - part

            @pl.loop(low, high)
            def _(i):
                multiply(2 * i + 1, 1)
                activate(2 * i, 0)
                multiply(2 * i + 2, 0)
                activate(2 * i + 1, 1)

            if part == 1:
                multiply(tiles1 - 1, 1)
                activate(tiles1 - 2, 0)
                activate(tiles1 - 1, 1)
            copy_hidden(c, part).start()

    q_at = iota((QUERY_PER_KEY * TILE, TILE), 0) % TILE
    s_at = iota((QUERY_PER_KEY * TILE, TILE), 1)
    allowed = (q_at // img_most == s_at // img_most) & (s_at <= q_at)

    def finish(c):
        size = sizes[c]
        for part in range(2):
            copy_hidden(c, part).wait_recv()
        pos_hot = jnp.where(iota((size, TILE), 1) == chunk_rows[c][1], 1.0, 0.0).astype(BF16)
        terms = jnp.dot(pos_hot, table[...], preferred_element_type=F32)
        w = HEAD_SIZE
        cos = terms[:, :w] + terms[:, w : 2 * w] + terms[:, 2 * w : 3 * w]
        sin = terms[:, 3 * w : 4 * w] + terms[:, 4 * w : 5 * w] + terms[:, 5 * w :]

        gains = rms_gain[...].reshape(1, -1).astype(F32)

        @pl.loop(0, size // 16, unroll=2)
        def _(r):
            at = pl.ds(pl.multiple_of(firsts[c] + r * 16, 16), 16)
            to = pl.ds(pl.multiple_of(r * 16, 16), 16)
            total = jnp.zeros((16, 1), F32)
            for h in range(2):
                x = hidden[h, at, :].astype(F32)
                total = total + jnp.sum(x * x, axis=-1, keepdims=True)
            scale = lax.rsqrt(total * (1.0 / (2 * half_cols)) + rms_epsilon)
            for h in range(2):
                x = hidden[h, at, :].astype(F32)
                g = gains[:, h * half_cols : (h + 1) * half_cols]
                rms_normed[to, h * half_cols : (h + 1) * half_cols] = (x * scale * g).astype(BF16)

        @pl.loop(0, tiles2)
        def _(j):
            if c == 0:
                w2_copy(j).wait()
            cols = pl.ds(pl.multiple_of(j * COL_TILE, COL_TILE), COL_TILE)
            proj[:size, cols] = jnp.dot(rms_normed[:size], w2[:, cols], preferred_element_type=F32)

        def head(first, h, rotate):
            v = proj[first : first + TILE, h * w : (h + 1) * w]
            if rotate:
                v = v * cos[first : first + TILE] + pltpu.roll(v, w // 2, 1) * sin[first : first + TILE]
            return v.astype(BF16)

        for first in range(0, size, TILE):
            for g in range(groups):
                h0 = g * (QUERY_PER_KEY + 2)
                q = jnp.concatenate(
                    [head(first, h0 + i, True) for i in range(QUERY_PER_KEY)], axis=0
                )
                k = head(first, h0 + QUERY_PER_KEY, True)
                v = head(first, h0 + QUERY_PER_KEY + 1, False)
                scores = lax.dot_general(
                    q, k, (((1,), (1,)), ((), ())), preferred_element_type=F32
                ) * np.float32(HEAD_SIZE ** (-0.5))
                scores = jnp.where(allowed, scores, -1e30)
                weights = jnp.exp(scores - jnp.max(scores, axis=-1, keepdims=True))
                probs = (weights / jnp.sum(weights, axis=-1, keepdims=True)).astype(BF16)
                got = jnp.dot(probs, v, preferred_element_type=F32).astype(BF16)
                for i in range(QUERY_PER_KEY):
                    a = (g * QUERY_PER_KEY + i) * w
                    outbox[firsts[c] + first : firsts[c] + first + TILE, a : a + w] = got[
                        i * TILE : (i + 1) * TILE
                    ]
        for o in range(firsts[c] // block, (firsts[c] + size) // block):
            if o < senders - 1:
                copy_block(o).start()
        if c == chunks - 1:
            inbox[box_rows - block :, :] = outbox[box_rows - block :, :]

    for c in range(chunks):
        project(c)
        finish(c)

    t_at = iota((TILE, images), 0)
    image_at = iota((TILE, images), 1)
    place_of = []
    for t in range(tiles_dev):
        hit = (image_at // img_tile == t) & (t_at >= my_off_row) & (t_at < my_off_row + my_row)
        at = jnp.where(hit, slot_row * img_most + (t_at - my_off_row) + 1, 0)
        place_of.append(lane_sum(at) - 1)

    def out_copy(t):
        at = pl.ds(t * TILE, TILE)
        return pltpu.make_async_copy(placed.at[at], out.at[at], out_sem.at[t])

    for o in range(senders - 1):
        copy_block(o).wait_recv()
    for t in range(tiles_dev):
        select = jnp.where(iota((TILE, box_rows), 1) == place_of[t], 1.0, 0.0).astype(BF16)
        placed[t * TILE : (t + 1) * TILE, :] = jnp.dot(
            select, inbox[...], preferred_element_type=F32
        ).astype(BF16)
        out_copy(t).start()
    for t in range(tiles_dev):
        out_copy(t).wait()

    for i in range(2):
        norm_copy(i).wait_send()
    for c in range(chunks):
        for part in range(2):
            copy_hidden(c, part).wait_send()
    for o in range(senders - 1):
        copy_block(o).wait_send()


def local(
    patches, ln_gain, ln_bias, w_proj, proj_bias, rms_gain, w_qkv, image_counts, source_shift
):
    senders = lax.axis_size("dp")
    order = shift_order(senders)
    half, d_vit = patches.shape
    rows = 2 * half
    half_cols = w_proj.shape[1]
    qkv_cols = w_qkv.shape[1]
    groups = qkv_cols // ((QUERY_PER_KEY + 2) * HEAD_SIZE)
    out_cols = groups * QUERY_PER_KEY * HEAD_SIZE
    images = source_shift.shape[0]
    img_most = TILE // (images // (rows // TILE))
    pair_slots = (images + senders - 1) // senders
    box_rows = senders * pair_slots * img_most
    sizes = chunk_list(box_rows)
    chunks = len(sizes)
    size = max(sizes)
    vmem = pl.BlockSpec(memory_space=pltpu.VMEM)
    hbm = pl.BlockSpec(memory_space=pl.ANY)
    dma = pltpu.SemaphoreType.DMA
    return pl.pallas_call(
        functools.partial(kernel, senders, order),
        out_shape=jax.ShapeDtypeStruct((rows, out_cols), BF16),
        in_specs=[vmem] * 7 + [hbm] * 3,
        out_specs=hbm,
        scratch_shapes=[
            pltpu.VMEM((half, d_vit), BF16),
            pltpu.VMEM(w_proj.shape, BF16),
            pltpu.VMEM(w_qkv.shape, BF16),
            pltpu.VMEM((rows, d_vit), BF16),
            pltpu.VMEM((size, d_vit), BF16),
            pltpu.VMEM((2, box_rows, half_cols), BF16),
            pltpu.VMEM((size, 2 * half_cols), BF16),
            pltpu.VMEM((2, size, COL_TILE), F32),
            pltpu.VMEM((1, half_cols), F32),
            pltpu.VMEM((size, qkv_cols), F32),
            pltpu.VMEM((box_rows, out_cols), BF16),
            pltpu.VMEM((box_rows, out_cols), BF16),
            pltpu.VMEM((rows, out_cols), BF16),
            dma((2,)),
            dma((rows // TILE,)),
            dma((half_cols // COL_TILE,)),
            dma((qkv_cols // COL_TILE,)),
            dma((2,)),
            dma((2,)),
            dma((2 * chunks,)),
            dma((2 * chunks,)),
            dma((senders,)),
            dma((senders,)),
        ],
        compiler_params=pltpu.CompilerParams(
            collective_id=0, has_side_effects=True, vmem_limit_bytes=60 * 1024 * 1024
        ),
        name="projector_attention",
    )(
        ln_gain,
        ln_bias,
        proj_bias,
        rms_gain,
        image_counts.T,
        source_shift,
        jnp.asarray(rotary_parts()),
        patches,
        w_proj,
        w_qkv,
    )


def solution(mesh):
    in_specs = (
        P(("dp", "mp"), None),
        P(),
        P(),
        P(None, "mp"),
        P("mp"),
        P(),
        P(None, "mp"),
        P(),
        P(),
    )
    out_specs = P("dp", "mp")
    return jax.shard_map(local, mesh=mesh, in_specs=in_specs, out_specs=out_specs, check_vma=False)
```
